32 devices in a mesh: gx: 2 (over x), gy: 4 (over z), gz: 4 (over y, core).
Axes of the slice: x: 2, y: 2, z: 4, core: 2. Of those that a mesh axis runs over, the one named last changes fastest.
Arguments:
- calcium: float32 [8, 64, 128, 512], P(None, 'gx', 'gz', 'gy'), may hold values from 0.1 to 3
- activation: float32 [8, 64, 128, 512], P(None, 'gx', 'gz', 'gy'), may hold values from 0 to 1
- element_first: int32 [64], replicated, may hold values from 0 to 15, as said below
- offset_first: float32 [64], replicated, may hold values from 0.1 to 0.9
- element_second: int32 [512], replicated, may hold values from 0 to 127, as said below
- offset_second: float32 [512], replicated, may hold values from 0.1 to 0.9
- element_third: int32 [128], replicated, may hold values from 0 to 31, as said below
- offset_third: float32 [128], replicated, may hold values from 0.1 to 0.9
- troponin: float32 [16, 32, 128], P('gx', ('gy', 'gz')), may hold values from 0 to 1
- tension: float32 [16, 32, 128], P('gx', ('gy', 'gz')), may hold values from 0 to 2
- unbind_rate: float32 [16, 32, 128], P('gx', ('gy', 'gz')), may hold values from 0.2 to 2
- relax_rate: float32 [16, 32, 128], P('gx', ('gy', 'gz')), may hold values from 0.5 to 4
Outputs:
- bound_fraction: float32 [16, 32, 128], P('gx', ('gy', 'gz'))
- active_tension: float32 [16, 32, 128], P('gx', ('gy', 'gz'))
The draws below stay inside these ranges and needn't reach their ends.
Inputs may be any that keep to these rules, and one draw needn't show every extreme that they name: `element_first`: never falling; the cells of each aligned block of 32 cells belong to that block's own 8 elements, each element holding at least one cell. `element_second`: never falling; the cells of each aligned block of 128 cells belong to that block's own 32 elements, each element holding at least one cell. `element_third`: never falling; the cells of each aligned block of 8 cells belong to that block's own 2 elements, each element holding at least one cell.
All inputs are finite; a program needn't handle non-finite values.
Results may differ from the reference program's by a relative error of at most 0.00005.
Values sent between devices are 32-bit elements.
A program may use at most 64 MiB of HBM per device.

```python
import math
import jax
import jax.numpy as jnp
from jax import lax

EX_DEV = 8
EY_DEV = 32
EZ_BLK = 2
SUB = 8
FX_BLK = 32
FY_BLK = 128
FZ_BLK = 8
NXC = 16
NYC = 128
NZC = 32
NXF = 64
NYF = 512
NZF = 128


def block_elements(key, blocks, cells, elements):

    def single(block_key):
        scores = jax.random.permutation(block_key, cells - 1) + 1
        cut_points = jnp.sort(scores[:elements - 1])
        places = jnp.arange(cells)
        return jnp.sum((places[:, None] >= cut_points[None, :]).astype(jnp.int32), axis=1)
    block_keys = jax.random.split(key, blocks)
    within = jax.vmap(single)(block_keys)
    offsets = elements * jnp.arange(blocks)[:, None]
    return (within + offsets).reshape(-1).astype(jnp.int32)


def draw_element_first(key, part):
    return block_elements(jax.random.fold_in(key, 11), NXF // FX_BLK, FX_BLK, EX_DEV)


def draw_element_second(key, part):
    return block_elements(jax.random.fold_in(key, 23), NYF // FY_BLK, FY_BLK, EY_DEV)


def draw_element_third(key, part):
    return block_elements(jax.random.fold_in(key, 37), NZF // FZ_BLK, FZ_BLK, EZ_BLK)


def block_scale(rng, extent, cuts, least, largest):
    level, own = 1.0, jax.random.fold_in(rng, 6)
    for dim, shards_of in cuts:
        draws = jnp.exp(jax.random.uniform(jax.random.fold_in(own, dim), (shards_of,), jnp.float32, least / len(cuts), largest / len(cuts)))
        level = level * jnp.repeat(draws, extent[dim] // shards_of).reshape([-1 if axis == dim else 1 for axis in range(len(extent))])
    return level


def setup_inputs(seed: int = 0) -> dict:
    streams_of = jax.random.split(jax.random.key(seed), 13)
    return {
        "calcium": jnp.clip(jnp.exp(math.log(3.0) - 3.4011974 * jax.random.uniform(streams_of[0], (SUB, NXF, NZF, NYF), jnp.float32) ** block_scale(streams_of[0], (SUB, NXF, NZF, NYF), ((1, 2), (2, 4), (3, 4)), -0.2, 0.2)), 0.1, 3.0),
        "activation": jnp.clip(1.0 * jax.random.uniform(streams_of[1], (SUB, NXF, NZF, NYF), jnp.float32) ** block_scale(streams_of[1], (SUB, NXF, NZF, NYF), ((1, 2), (2, 4), (3, 4)), -0.2, 0.2), 0.0, 1.0),
        "element_first": draw_element_first(jax.random.fold_in(streams_of[12], 71), 0),
        "offset_first": jnp.clip(jax.random.uniform(streams_of[3], (NXF,), jnp.float32, 0.1, 0.9), 0.1, 0.9),
        "element_second": draw_element_second(jax.random.fold_in(streams_of[12], 71), 0),
        "offset_second": jnp.clip(jax.random.uniform(streams_of[5], (NYF,), jnp.float32, 0.1, 0.9), 0.1, 0.9),
        "element_third": draw_element_third(jax.random.fold_in(streams_of[12], 71), 0),
        "offset_third": jnp.clip(jax.random.uniform(streams_of[7], (NZF,), jnp.float32, 0.1, 0.9), 0.1, 0.9),
        "troponin": jnp.clip(1.0 * jax.random.uniform(streams_of[8], (NXC, NZC, NYC), jnp.float32) ** block_scale(streams_of[8], (NXC, NZC, NYC), ((0, 2), (1, 16)), -0.2, 0.2), 0.0, 1.0),
        "tension": jnp.clip(2.0 * jax.random.uniform(streams_of[9], (NXC, NZC, NYC), jnp.float32) ** block_scale(streams_of[9], (NXC, NZC, NYC), ((0, 2), (1, 16)), -0.2, 0.2), 0.0, 2.0),
        "unbind_rate": jnp.clip(jnp.exp(math.log(2.0) - 2.3025851 * jax.random.uniform(streams_of[10], (NXC, NZC, NYC), jnp.float32) ** block_scale(streams_of[10], (NXC, NZC, NYC), ((0, 2), (1, 16)), -0.2, 0.2)), 0.2, 2.0),
        "relax_rate": jnp.clip(jnp.exp(math.log(4.0) - 2.0794415 * jax.random.uniform(streams_of[11], (NXC, NZC, NYC), jnp.float32) ** block_scale(streams_of[11], (NXC, NZC, NYC), ((0, 2), (1, 16)), -0.2, 0.2)), 0.5, 4.0),
    }


highest = lax.Precision.HIGHEST
step_size = 0.2
bind_rate = 2.0
peak_tension = 2.0
half_square = 0.25


def weights(element, offset, count):
    node_ids = jnp.arange(count, dtype=jnp.int32)
    inside = element[None, :] == node_ids[:, None]
    following = element[None, :] + 1 == node_ids[:, None]
    raw_weights = jnp.where(inside, 1.0 - offset[None, :], 0.0) + jnp.where(following, offset[None, :], 0.0)
    return raw_weights / jnp.sum(raw_weights, axis=1, keepdims=True)


def restrict(field, weight_row, weight_depth, weight_col):
    section = jnp.einsum("ai,izy->azy", weight_row, field, precision=highest)
    section = jnp.einsum("bz,azy->aby", weight_depth, section, precision=highest)
    return jnp.einsum("cy,aby->abc", weight_col, section, precision=highest)


def reference(calcium, activation, element_first, offset_first, element_second, offset_second, element_third, offset_third, troponin, tension, unbind_rate, relax_rate):
    weight_row = weights(element_first, offset_first, NXC)
    weight_col = weights(element_second, offset_second, NYC)
    weight_depth = weights(element_third, offset_third, NZC)

    def single(index):
        return (restrict(calcium[index], weight_row, weight_depth, weight_col),
                restrict(activation[index], weight_row, weight_depth, weight_col))

    drive_calcium, drive_activation = lax.map(single, jnp.arange(SUB, dtype=jnp.int32))
    bound = troponin
    active = tension
    for substep in range(SUB):
        calcium_now = drive_calcium[substep]
        squared = calcium_now * calcium_now
        binding = squared / (squared + half_square)
        bound = bound + step_size * (bind_rate * binding * (1.0 - bound) - unbind_rate * bound)
        active = active + step_size * relax_rate * (peak_tension * drive_activation[substep] * bound - active)
    return bound, active
```

```python
import functools

import jax
import jax.numpy as jnp
from jax import lax
from jax.experimental import pallas as pl
from jax.experimental.pallas import tpu as pltpu
from jax.sharding import PartitionSpec as P

step_size = 0.2
bind_rate = 2.0
peak_tension = 2.0
half_square = 0.25
f32 = jnp.float32
bf16 = jnp.bfloat16
MESH = pl.DeviceIdType.MESH
CHUNKS = 2


def split(x):
    high = x.astype(bf16)
    return high, (x - high.astype(f32)).astype(bf16)


def node_weights(element, offset, node):
    raw = jnp.where(element == node, 1.0 - offset, 0.0) + jnp.where(
        element + 1 == node, offset, 0.0
    )
    total = jnp.sum(raw, axis=1, keepdims=True)
    return raw, jnp.where(total > 0.0, total, 1.0)


def iota(shape, dim):
    return lax.broadcasted_iota(jnp.int32, shape, dim)


def kernel(
    calcium,
    activation,
    e1,
    o1,
    e2,
    o2,
    e3,
    o3,
    troponin,
    tension,
    unbind,
    relax,
    out_bound,
    out_active,
    xc,
    xa,
    main,
    edge,
    got_main,
    got_third,
    got_first,
    got_corner,
    load_sem,
    send_main,
    send_edge,
    recv_main,
    recv_third,
    recv_first,
    recv_corner,
    *,
    sizes,
):
    nx, ny, nz = sizes
    subs, rows, depth, cols = xc.shape
    nodes_x, per_block, all_y = troponin.shape
    nodes_y = all_y // ny
    blocks = nz
    slab = per_block * blocks
    gx, gy, gz = lax.axis_index("gx"), lax.axis_index("gy"), lax.axis_index("gz")
    chunk = subs // CHUNKS

    def load(t):
        return (
            pltpu.make_async_copy(calcium.at[t], xc.at[t], load_sem.at[0, t]),
            pltpu.make_async_copy(activation.at[t], xa.at[t], load_sem.at[1, t]),
        )

    for t in range(subs):
        for copy in load(t):
            copy.start()

    barrier = pltpu.get_barrier_semaphore()
    has_next_x = gx + 1 < nx
    has_next_z = gz + 1 < nz
    own = gy == gz
    from_third = jnp.logical_and(gz == 0, gy > 0)
    from_first = gx > 0
    from_corner = jnp.logical_and(from_third, from_first)
    for s in range(ny):

        def greet(dx, dz, s=s):
            pl.semaphore_signal(
                barrier, inc=1, device_id=(gx - dx, s, gy - dz), device_id_type=MESH
            )

        @pl.when(jnp.logical_not(jnp.logical_and(s == gy, own)))
        def _():
            greet(0, 0)

        @pl.when(jnp.logical_and(from_third, jnp.logical_not(jnp.logical_and(s == gy, gy - 1 == gz))))
        def _():
            greet(0, 1)

        @pl.when(from_first)
        def _():
            greet(1, 0)

        @pl.when(from_corner)
        def _():
            greet(1, 1)

    row_count = (slab + 1) * nodes_x + 16
    r = iota((row_count, 1), 0)
    inner = r < (slab + 1) * nodes_x
    tail = r - (slab + 1) * nodes_x
    node_a = jnp.where(inner, r % nodes_x, nodes_x)
    node_b = jnp.where(inner, r // nodes_x, per_block * (tail % 8) + tail // 8)
    raw, total = node_weights(e1[...], o1[...], node_a + gx * nodes_x)
    wide = rows * depth
    pick = (
        iota((raw.shape[1], wide), 0) == gx * rows + iota((raw.shape[1], wide), 1) // depth
    ).astype(f32)
    weight_x = jnp.dot(
        raw / total, pick, precision=lax.Precision.HIGHEST, preferred_element_type=f32
    )
    raw, total = node_weights(e3[...], o3[...], node_b + gz * slab)
    pick = (
        iota((raw.shape[1], wide), 0) == gz * depth + iota((raw.shape[1], wide), 1) % depth
    ).astype(f32)
    weight_z = jnp.dot(
        raw / total, pick, precision=lax.Precision.HIGHEST, preferred_element_type=f32
    )
    k_high, k_low = split(weight_x * weight_z)
    k_both = jnp.concatenate([k_high, k_low], axis=0)

    lanes = 2 * per_block * nodes_y
    n = iota((lanes, 1), 0)
    mine = pl.ds(pl.multiple_of(gy * cols, cols), cols)
    spread = []
    for ghost in range(2):
        node = gy * nodes_y + (nodes_y if ghost else n % nodes_y)
        node = node + jnp.zeros_like(n)
        total = node_weights(e2[...], o2[...], node)[1]
        weight = node_weights(e2[:, mine], o2[:, mine], node)[0] / total
        if ghost:
            weight = jnp.where(n % nodes_y == 0, weight, 0.0)
        spread.append(
            jnp.concatenate(
                [
                    jnp.where(n // nodes_y == f * per_block + b, weight, 0.0)
                    for b in range(per_block)
                    for f in range(2)
                ],
                axis=1,
            )
        )
    y_high, y_low = split(jnp.concatenate(spread, axis=0))

    def to_message(values):
        high, low = split(values)
        dims = (((1,), (1,)), ((), ()))
        dot = functools.partial(
            lax.dot_general, dimension_numbers=dims, preferred_element_type=f32
        )
        return dot(high, y_high) + dot(low, y_high) + dot(high, y_low)

    def part(c):
        first = c * chunk * nodes_x
        last = (c + 1) * chunk * nodes_x + (nodes_x if c == CHUNKS - 1 else 0)
        return pl.ds(first, last - first)

    def main_copy(q, c):
        return pltpu.make_async_remote_copy(
            src_ref=main.at[q, part(c)],
            dst_ref=got_main.at[gy, part(c)],
            send_sem=send_main.at[q, c],
            recv_sem=recv_main.at[gy, c],
            device_id=(gx, gz, q),
            device_id_type=MESH,
        )

    def third_copy(c):
        return pltpu.make_async_remote_copy(
            src_ref=main.at[blocks, part(c)],
            dst_ref=got_third.at[gy, part(c)],
            send_sem=send_main.at[blocks, c],
            recv_sem=recv_third.at[gy, c],
            device_id=(gx, gz + 1, 0),
            device_id_type=MESH,
        )

    def first_copy(q):
        return pltpu.make_async_remote_copy(
            src_ref=edge.at[q],
            dst_ref=got_first.at[gy],
            send_sem=send_edge.at[q],
            recv_sem=recv_first.at[gy],
            device_id=(gx + 1, gz, q),
            device_id_type=MESH,
        )

    def corner_copy():
        return pltpu.make_async_remote_copy(
            src_ref=edge.at[blocks],
            dst_ref=got_corner.at[gy],
            send_sem=send_edge.at[blocks],
            recv_sem=recv_corner.at[gy],
            device_id=(gx + 1, gz + 1, 0),
            device_id_type=MESH,
        )

    third_here = jnp.logical_and(gz == 0, gy == 1)
    third_away = jnp.logical_and(has_next_z, jnp.logical_not(third_here))

    def each_main(c, do):
        for q in range(blocks):

            @pl.when(jnp.logical_not(jnp.logical_and(own, gz == q)))
            def _(q=q):
                do(main_copy(q, c))

        @pl.when(third_away)
        def _():
            do(third_copy(c))

    def each_edge(do):
        @pl.when(has_next_x)
        def _():
            for q in range(blocks):
                do(first_copy(q))

        @pl.when(jnp.logical_and(has_next_x, has_next_z))
        def _():
            do(corner_copy())

    packed = None
    tile = nodes_x
    for c in range(CHUNKS):
        gathered = []
        for t in range(c * chunk, (c + 1) * chunk):
            for copy in load(t):
                copy.wait()
            field = jnp.concatenate(
                [xc[t].reshape(wide, cols), xa[t].reshape(wide, cols)], axis=1
            )
            high, low = split(field)
            both = jnp.dot(k_both, high, preferred_element_type=f32)
            node = (
                both[:row_count]
                + both[row_count:]
                + jnp.dot(k_high, low, preferred_element_type=f32)
            )
            sides = []
            for k in range(per_block):
                pieces = []
                for q in range(blocks + 1):
                    b = q * per_block + k
                    if b <= slab:
                        pieces.append(node[b * tile : (b + 1) * tile])
                    else:
                        pieces.append(jnp.zeros((tile, 2 * cols), f32))
                base = (slab + 1) * tile + 8 * k
                pieces.append(node[base : base + 8])
                sides.append(jnp.concatenate(pieces, axis=0))
            gathered.append(jnp.concatenate(sides, axis=1))
        result = to_message(jnp.concatenate(gathered, axis=0))
        per = (blocks + 1) * tile + 8
        for k, t in enumerate(range(c * chunk, (c + 1) * chunk)):
            values = result[k * per : (k + 1) * per]
            for q in range(blocks + 1):
                main[q, t * tile : (t + 1) * tile] = values[q * tile : (q + 1) * tile, :lanes]
                row = (blocks + 1) * tile + q
                edge[q, t : t + 1] = values[row : row + 1, :lanes]
                edge[q, subs + t : subs + t + 1] = values[row : row + 1, lanes:]
            ghost = values[: (blocks + 1) * tile, lanes:]
            if t:
                ghost = pltpu.roll(ghost, t, 1)
            packed = ghost if packed is None else packed + ghost
        if c == CHUNKS - 1:
            for q in range(blocks + 1):
                main[q, subs * tile : (subs + 1) * tile] = packed[q * tile : (q + 1) * tile]
        if c == 0:
            count = blocks + has_next_z.astype(jnp.int32)
            count = count * jnp.where(has_next_x, 2, 1)
            count = count - jnp.logical_or(own, third_here).astype(jnp.int32)
            pl.semaphore_wait(barrier, count)
        each_main(c, lambda copy: copy.start())
    each_edge(lambda copy: copy.start())

    @pl.when(own)
    def _():
        got_main[gy] = main[gz]

    @pl.when(third_here)
    def _():
        got_third[gy] = main[blocks]

    first_rows = [pl.ds(t * tile, 1) for t in range(subs)]
    for s in range(ny):

        @pl.when(jnp.logical_not(jnp.logical_and(own, gy == s)))
        def _(s=s):
            for c in range(CHUNKS):
                pltpu.make_async_remote_copy(
                    src_ref=main.at[0, part(c)],
                    dst_ref=got_main.at[s, part(c)],
                    send_sem=send_main.at[0, c],
                    recv_sem=recv_main.at[s, c],
                    device_id=(gx, gy, gz),
                    device_id_type=MESH,
                ).wait_recv()

    @pl.when(from_third)
    def _():
        for s in range(ny):

            @pl.when(jnp.logical_not(jnp.logical_and(gy == 1, jnp.logical_and(gz == 0, s == gy)) & (gz == gy - 1)))
            def _(s=s):
                for c in range(CHUNKS):
                    pltpu.make_async_remote_copy(
                        src_ref=main.at[0, part(c)],
                        dst_ref=got_third.at[s, part(c)],
                        send_sem=send_main.at[0, c],
                        recv_sem=recv_third.at[s, c],
                        device_id=(gx, gy, gz),
                        device_id_type=MESH,
                    ).wait_recv()

            got_main[s] = got_main[s] + got_third[s]

    def add_edge(source, sem, s):
        pltpu.make_async_remote_copy(
            src_ref=edge.at[0],
            dst_ref=source.at[s],
            send_sem=send_edge.at[0],
            recv_sem=sem.at[s],
            device_id=(gx, gy, gz),
            device_id_type=MESH,
        ).wait_recv()
        ghost = jnp.zeros((1, lanes), f32)
        for t in range(subs):
            got_main[s, first_rows[t]] = got_main[s, first_rows[t]] + source[s, t : t + 1]
            moved = source[s, subs + t : subs + t + 1]
            ghost = ghost + (pltpu.roll(jnp.broadcast_to(moved, (8, lanes)), t, 1)[:1] if t else moved)
        last = pl.ds(subs * tile, 1)
        got_main[s, last] = got_main[s, last] + ghost

    @pl.when(from_first)
    def _():
        for s in range(ny):
            add_edge(got_first, recv_first, s)

    @pl.when(from_corner)
    def _():
        for s in range(ny):
            add_edge(got_corner, recv_corner, s)

    lane = iota((tile, lanes), 1)
    lane_y = iota((tile, all_y), 1)
    ghosts = [got_main[s, subs * tile : (subs + 1) * tile] for s in range(ny - 1)]
    bound = [troponin[:, k, :] for k in range(per_block)]
    active = [tension[:, k, :] for k in range(per_block)]
    unbind_rate = [unbind[:, k, :] for k in range(per_block)]
    relax_rate = [relax[:, k, :] for k in range(per_block)]
    for t in range(subs):
        pieces = []
        for s in range(ny):
            value = got_main[s, t * tile : (t + 1) * tile]
            if s:
                moved = pltpu.roll(ghosts[s - 1], lanes - t, 1) if t else ghosts[s - 1]
                value = value + jnp.where(lane % nodes_y == 0, moved, 0.0)
            pieces.append(value)

        def drive(f, k):
            at = (f * per_block + k) * nodes_y
            total = None
            for s in range(ny):
                shift = (s * nodes_y - at) % lanes
                moved = pltpu.roll(pieces[s], shift, 1) if shift else pieces[s]
                total = moved if total is None else jnp.where(lane_y // nodes_y == s, moved, total)
            return total

        for k in range(per_block):
            squared = drive(0, k)
            squared = squared * squared
            binding = squared / (squared + half_square)
            bound[k] = bound[k] + step_size * (
                bind_rate * binding * (1.0 - bound[k]) - unbind_rate[k] * bound[k]
            )
            active[k] = active[k] + step_size * relax_rate[k] * (
                peak_tension * drive(1, k) * bound[k] - active[k]
            )
    for k in range(per_block):
        out_bound[:, k, :] = bound[k]
        out_active[:, k, :] = active[k]

    for c in range(CHUNKS):
        each_main(c, lambda copy: copy.wait_send())
    each_edge(lambda copy: copy.wait_send())


def per_device(calcium, activation, e1, o1, e2, o2, e3, o3, troponin, tension, unbind, relax, *, sizes):
    nx, ny, nz = sizes
    subs, rows, depth, cols = calcium.shape
    nodes_x, per_block, all_y = troponin.shape
    lanes = 2 * per_block * (all_y // ny)
    blocks = nz
    long = (subs + 1) * nodes_x
    vmem = pl.BlockSpec(memory_space=pltpu.VMEM)
    hbm = pl.BlockSpec(memory_space=pltpu.MemorySpace.HBM)
    dma = pltpu.SemaphoreType.DMA
    flat = [x.reshape(1, -1) for x in (e1, o1, e2, o2, e3, o3)]
    shape = jax.ShapeDtypeStruct(troponin.shape, f32)
    return pl.pallas_call(
        functools.partial(kernel, sizes=sizes),
        out_shape=(shape, shape),
        in_specs=[hbm] * 2 + [vmem] * 10,
        out_specs=(vmem, vmem),
        scratch_shapes=[
            pltpu.VMEM(calcium.shape, f32),
            pltpu.VMEM(calcium.shape, f32),
            pltpu.VMEM((blocks + 1, long, lanes), f32),
            pltpu.VMEM((blocks + 1, 2 * subs, lanes), f32),
            pltpu.VMEM((ny, long, lanes), f32),
            pltpu.VMEM((ny, long, lanes), f32),
            pltpu.VMEM((ny, 2 * subs, lanes), f32),
            pltpu.VMEM((ny, 2 * subs, lanes), f32),
            dma((2, subs)),
            dma((blocks + 1, CHUNKS)),
            dma((blocks + 1,)),
            dma((ny, CHUNKS)),
            dma((ny, CHUNKS)),
            dma((ny,)),
            dma((ny,)),
        ],
        compiler_params=pltpu.CompilerParams(
            collective_id=0, has_side_effects=True, vmem_limit_bytes=48 * 1024 * 1024
        ),
        name="restrict_steps",
    )(calcium, activation, *flat, troponin, tension, unbind, relax)


def solution(mesh):
    sizes = tuple(mesh.shape[name] for name in ("gx", "gy", "gz"))
    field = P(None, "gx", "gz", "gy")
    nodes = P("gx", ("gy", "gz"), None)
    return jax.shard_map(
        functools.partial(per_device, sizes=sizes),
        mesh=mesh,
        in_specs=(field, field, P(), P(), P(), P(), P(), P(), nodes, nodes, nodes, nodes),
        out_specs=(nodes, nodes),
        check_vma=False,
    )
```

```python
import functools

import jax
import jax.numpy as jnp
from jax import lax
from jax.experimental import pallas as pl
from jax.experimental.pallas import tpu as pltpu
from jax.sharding import PartitionSpec as P

step_size = 0.2
bind_rate = 2.0
peak_tension = 2.0
half_square = 0.25
f32 = jnp.float32
bf16 = jnp.bfloat16
MESH = pl.DeviceIdType.MESH
CHUNKS = 2


def split(x):
    high = x.astype(bf16)
    return high, (x - high.astype(f32)).astype(bf16)


def node_weights(element, offset, node):
    raw = jnp.where(element == node, 1.0 - offset, 0.0) + jnp.where(
        element + 1 == node, offset, 0.0
    )
    total = jnp.sum(raw, axis=1, keepdims=True)
    return raw, jnp.where(total > 0.0, total, 1.0)


def expand(weight, pick):
    high, low = split(weight)
    return jnp.dot(high, pick, preferred_element_type=f32) + jnp.dot(
        low, pick, preferred_element_type=f32
    )


def iota(shape, dim):
    return lax.broadcasted_iota(jnp.int32, shape, dim)


def kernel(
    calcium,
    activation,
    *refs,
    sizes,
):
    small = refs[:10]
    out_bound, out_active, xc, xa = refs[10:14]
    local = refs[14:24]
    (
        main,
        third,
        edge,
        got_main,
        got_third,
        got_first,
        got_corner,
        load_sem,
        small_sem,
        send_main,
        send_edge,
        recv_main,
        recv_third,
        recv_first,
        recv_corner,
    ) = refs[24:]
    e1, o1, e2, o2, e3, o3, troponin, tension, unbind, relax = local
    nx, ny, nz = sizes
    subs, rows, depth, cols = xc.shape
    nodes_x, per_block, all_y = troponin.shape
    nodes_y = all_y // ny
    blocks = nz
    slab = per_block * blocks
    gx, gy, gz = lax.axis_index("gx"), lax.axis_index("gy"), lax.axis_index("gz")
    chunk = subs // CHUNKS

    def load(t):
        return (
            pltpu.make_async_copy(calcium.at[t], xc.at[t], load_sem.at[0, t]),
            pltpu.make_async_copy(activation.at[t], xa.at[t], load_sem.at[1, t]),
        )

    fetches = [
        pltpu.make_async_copy(source, target, small_sem.at[i])
        for i, (source, target) in enumerate(zip(small, local))
    ]
    for copy in fetches:
        copy.start()
    for t in range(subs):
        for copy in load(t):
            copy.start()

    barrier = pltpu.get_barrier_semaphore()
    has_next_x = gx + 1 < nx
    has_next_z = gz + 1 < nz
    own = gy == gz
    from_third = jnp.logical_and(gz == 0, gy > 0)
    from_first = gx > 0
    from_corner = jnp.logical_and(from_third, from_first)
    for s in range(ny):

        def greet(dx, dz, s=s):
            pl.semaphore_signal(
                barrier, inc=1, device_id=(gx - dx, s, gy - dz), device_id_type=MESH
            )

        @pl.when(jnp.logical_not(jnp.logical_and(s == gy, own)))
        def _():
            greet(0, 0)

        @pl.when(jnp.logical_and(from_third, jnp.logical_not(jnp.logical_and(s == gy, gy - 1 == gz))))
        def _():
            greet(0, 1)

        @pl.when(from_first)
        def _():
            greet(1, 0)

        @pl.when(from_corner)
        def _():
            greet(1, 1)

    for copy in fetches[:6]:
        copy.wait()
    row_count = (slab + 1) * nodes_x + 16
    r = iota((row_count, 1), 0)
    inner = r < (slab + 1) * nodes_x
    tail = r - (slab + 1) * nodes_x
    node_a = jnp.where(inner, r % nodes_x, nodes_x)
    node_b = jnp.where(inner, r // nodes_x, per_block * (tail % 8) + tail // 8)
    raw, total = node_weights(e1[...], o1[...], node_a + gx * nodes_x)
    wide = rows * depth
    pick = (
        iota((raw.shape[1], wide), 0) == gx * rows + iota((raw.shape[1], wide), 1) // depth
    ).astype(bf16)
    weight_x = expand(raw / total, pick)
    raw, total = node_weights(e3[...], o3[...], node_b + gz * slab)
    pick = (
        iota((raw.shape[1], wide), 0) == gz * depth + iota((raw.shape[1], wide), 1) % depth
    ).astype(bf16)
    weight_z = expand(raw / total, pick)
    k_high, k_low = split(weight_x * weight_z)
    k_both = jnp.concatenate([k_high, k_low], axis=0)

    lanes = 2 * per_block * nodes_y
    n = iota((lanes, 1), 0)
    mine = pl.ds(pl.multiple_of(gy * cols, cols), cols)
    spread = []
    for ghost in range(2):
        node = gy * nodes_y + (nodes_y if ghost else n % nodes_y)
        node = node + jnp.zeros_like(n)
        total = node_weights(e2[...], o2[...], node)[1]
        weight = node_weights(e2[:, mine], o2[:, mine], node)[0] / total
        if ghost:
            weight = jnp.where(n % nodes_y == 0, weight, 0.0)
        spread.append(
            jnp.concatenate(
                [
                    jnp.where(n // nodes_y == f * per_block + b, weight, 0.0)
                    for b in range(per_block)
                    for f in range(2)
                ],
                axis=1,
            )
        )
    y_high, y_low = split(jnp.concatenate(spread, axis=0))

    def to_message(values):
        high, low = split(values)
        dims = (((1,), (1,)), ((), ()))
        dot = functools.partial(
            lax.dot_general, dimension_numbers=dims, preferred_element_type=f32
        )
        return dot(high, y_high) + dot(low, y_high) + dot(high, y_low)

    def part(c):
        first = c * chunk * nodes_x
        last = (c + 1) * chunk * nodes_x + (nodes_x if c == CHUNKS - 1 else 0)
        return pl.ds(first, last - first)

    def main_copy(q, c):
        return pltpu.make_async_remote_copy(
            src_ref=main.at[q, part(c)],
            dst_ref=got_main.at[gy, part(c)],
            send_sem=send_main.at[q, c],
            recv_sem=recv_main.at[gy, c],
            device_id=(gx, gz, q),
            device_id_type=MESH,
        )

    def third_part(c):
        step = chunk // per_block * nodes_x
        return pl.ds(c * step, step + (nodes_x if c == CHUNKS - 1 else 0))

    def third_copy(c):
        return pltpu.make_async_remote_copy(
            src_ref=third.at[third_part(c)],
            dst_ref=got_third.at[gy, third_part(c)],
            send_sem=send_main.at[blocks, c],
            recv_sem=recv_third.at[gy, c],
            device_id=(gx, gz + 1, 0),
            device_id_type=MESH,
        )

    def first_copy(q):
        return pltpu.make_async_remote_copy(
            src_ref=edge.at[q],
            dst_ref=got_first.at[gy],
            send_sem=send_edge.at[q],
            recv_sem=recv_first.at[gy],
            device_id=(gx + 1, gz, q),
            device_id_type=MESH,
        )

    def corner_copy():
        return pltpu.make_async_remote_copy(
            src_ref=edge.at[blocks],
            dst_ref=got_corner.at[gy],
            send_sem=send_edge.at[blocks],
            recv_sem=recv_corner.at[gy],
            device_id=(gx + 1, gz + 1, 0),
            device_id_type=MESH,
        )

    third_here = jnp.logical_and(gz == 0, gy == 1)
    third_away = jnp.logical_and(has_next_z, jnp.logical_not(third_here))

    def each_main(c, do):
        for q in range(blocks):

            @pl.when(jnp.logical_not(jnp.logical_and(own, gz == q)))
            def _(q=q):
                do(main_copy(q, c))

        @pl.when(third_away)
        def _():
            do(third_copy(c))

    def each_edge(do):
        @pl.when(has_next_x)
        def _():
            for q in range(blocks):
                do(first_copy(q))

        @pl.when(jnp.logical_and(has_next_x, has_next_z))
        def _():
            do(corner_copy())

    packed = pair = None
    tile = nodes_x
    for c in range(CHUNKS):
        gathered = []
        for t in range(c * chunk, (c + 1) * chunk):
            for copy in load(t):
                copy.wait()
            field = jnp.concatenate(
                [xc[t].reshape(wide, cols), xa[t].reshape(wide, cols)], axis=1
            )
            high, low = split(field)
            both = jnp.dot(k_both, high, preferred_element_type=f32)
            node = (
                both[:row_count]
                + both[row_count:]
                + jnp.dot(k_high, low, preferred_element_type=f32)
            )
            sides = []
            for k in range(per_block):
                pieces = []
                for q in range(blocks + 1):
                    b = q * per_block + k
                    if b <= slab:
                        pieces.append(node[b * tile : (b + 1) * tile])
                    else:
                        pieces.append(jnp.zeros((tile, 2 * cols), f32))
                base = (slab + 1) * tile + 8 * k
                pieces.append(node[base : base + 8])
                sides.append(jnp.concatenate(pieces, axis=0))
            gathered.append(jnp.concatenate(sides, axis=1))
        result = to_message(jnp.concatenate(gathered, axis=0))
        per = (blocks + 1) * tile + 8
        for k, t in enumerate(range(c * chunk, (c + 1) * chunk)):
            values = result[k * per : (k + 1) * per]
            for q in range(blocks):
                main[q, t * tile : (t + 1) * tile] = values[q * tile : (q + 1) * tile, :lanes]
            for q in range(blocks + 1):
                row = (blocks + 1) * tile + q
                edge[q, t : t + 1] = values[row : row + 1, :lanes]
            above = values[blocks * tile : (blocks + 1) * tile, :lanes]
            place = t % per_block
            pair = pltpu.roll(above, place * nodes_y, 1) + pair if place else above
            if place == per_block - 1:
                at = t // per_block * tile
                third[at : at + tile] = pair
            ghost = values[:, lanes:]
            if t:
                ghost = pltpu.roll(ghost, t, 1)
            packed = ghost if packed is None else packed + ghost
        if c == CHUNKS - 1:
            for q in range(blocks):
                main[q, subs * tile : (subs + 1) * tile] = packed[q * tile : (q + 1) * tile]
            at = subs // per_block * tile
            third[at : at + tile] = packed[blocks * tile : (blocks + 1) * tile]
            for q in range(blocks + 1):
                row = (blocks + 1) * tile + q
                edge[q, subs : subs + 1] = packed[row : row + 1]
        if c == 0:
            count = blocks + has_next_z.astype(jnp.int32)
            count = count * jnp.where(has_next_x, 2, 1)
            count = count - jnp.logical_or(own, third_here).astype(jnp.int32)
            pl.semaphore_wait(barrier, count)
        each_main(c, lambda copy: copy.start())
    each_edge(lambda copy: copy.start())

    @pl.when(own)
    def _():
        got_main[gy] = main[gz]

    @pl.when(third_here)
    def _():
        got_third[gy] = third[...]

    for s in range(ny):

        @pl.when(jnp.logical_not(jnp.logical_and(own, gy == s)))
        def _(s=s):
            for c in range(CHUNKS):
                pltpu.make_async_remote_copy(
                    src_ref=main.at[0, part(c)],
                    dst_ref=got_main.at[s, part(c)],
                    send_sem=send_main.at[0, c],
                    recv_sem=recv_main.at[s, c],
                    device_id=(gx, gy, gz),
                    device_id_type=MESH,
                ).wait_recv()

    @pl.when(from_third)
    def _():
        for s in range(ny):

            @pl.when(jnp.logical_not(jnp.logical_and(gy == 1, jnp.logical_and(gz == 0, s == gy)) & (gz == gy - 1)))
            def _(s=s):
                for c in range(CHUNKS):
                    pltpu.make_async_remote_copy(
                        src_ref=third.at[third_part(c)],
                        dst_ref=got_third.at[s, third_part(c)],
                        send_sem=send_main.at[0, c],
                        recv_sem=recv_third.at[s, c],
                        device_id=(gx, gy, gz),
                        device_id_type=MESH,
                    ).wait_recv()

            first_block = iota((tile, lanes), 1) // nodes_y % per_block == 0
            for t in range(subs):
                at = t // per_block * tile
                moved = got_third[s, at : at + tile]
                place = t % per_block
                if place:
                    moved = pltpu.roll(moved, lanes - place * nodes_y, 1)
                rows_t = pl.ds(t * tile, tile)
                got_main[s, rows_t] = got_main[s, rows_t] + jnp.where(first_block, moved, 0.0)
            at = subs // per_block * tile
            rows_t = pl.ds(subs * tile, tile)
            got_main[s, rows_t] = got_main[s, rows_t] + got_third[s, at : at + tile]

    def add_edge(source, sem, s):
        pltpu.make_async_remote_copy(
            src_ref=edge.at[0],
            dst_ref=source.at[s],
            send_sem=send_edge.at[0],
            recv_sem=sem.at[s],
            device_id=(gx, gy, gz),
            device_id_type=MESH,
        ).wait_recv()
        for t in range(subs + 1):
            at = pl.ds(t * tile, 1)
            got_main[s, at] = got_main[s, at] + source[s, t : t + 1]

    @pl.when(from_first)
    def _():
        for s in range(ny):
            add_edge(got_first, recv_first, s)

    @pl.when(from_corner)
    def _():
        for s in range(ny):
            add_edge(got_corner, recv_corner, s)

    for copy in fetches[6:]:
        copy.wait()
    lane = iota((tile, lanes), 1)
    lane_y = iota((tile, all_y), 1)
    ghosts = [got_main[s, subs * tile : (subs + 1) * tile] for s in range(ny - 1)]
    bound = [troponin[:, k, :] for k in range(per_block)]
    active = [tension[:, k, :] for k in range(per_block)]
    unbind_rate = [unbind[:, k, :] for k in range(per_block)]
    relax_rate = [relax[:, k, :] for k in range(per_block)]
    for t in range(subs):
        pieces = []
        for s in range(ny):
            value = got_main[s, t * tile : (t + 1) * tile]
            if s:
                moved = pltpu.roll(ghosts[s - 1], lanes - t, 1) if t else ghosts[s - 1]
                value = value + jnp.where(lane % nodes_y == 0, moved, 0.0)
            pieces.append(value)

        def drive(f, k):
            at = (f * per_block + k) * nodes_y
            total = None
            for s in range(ny):
                shift = (s * nodes_y - at) % lanes
                moved = pltpu.roll(pieces[s], shift, 1) if shift else pieces[s]
                total = moved if total is None else jnp.where(lane_y // nodes_y == s, moved, total)
            return total

        for k in range(per_block):
            squared = drive(0, k)
            squared = squared * squared
            binding = squared / (squared + half_square)
            bound[k] = bound[k] + step_size * (
                bind_rate * binding * (1.0 - bound[k]) - unbind_rate[k] * bound[k]
            )
            active[k] = active[k] + step_size * relax_rate[k] * (
                peak_tension * drive(1, k) * bound[k] - active[k]
            )
    for k in range(per_block):
        out_bound[:, k, :] = bound[k]
        out_active[:, k, :] = active[k]

    for c in range(CHUNKS):
        each_main(c, lambda copy: copy.wait_send())
    each_edge(lambda copy: copy.wait_send())


def store_results(bound, active, out_bound, out_active, sem):
    copies = (
        pltpu.make_async_copy(bound, out_bound, sem.at[0]),
        pltpu.make_async_copy(active, out_active, sem.at[1]),
    )
    for copy in copies:
        copy.start()
    for copy in copies:
        copy.wait()


def per_device(calcium, activation, e1, o1, e2, o2, e3, o3, troponin, tension, unbind, relax, *, sizes):
    nx, ny, nz = sizes
    subs, rows, depth, cols = calcium.shape
    nodes_x, per_block, all_y = troponin.shape
    lanes = 2 * per_block * (all_y // ny)
    blocks = nz
    long = (subs + 1) * nodes_x
    short = (subs // per_block + 1) * nodes_x
    vmem = pl.BlockSpec(memory_space=pltpu.VMEM)
    hbm = pl.BlockSpec(memory_space=pltpu.MemorySpace.HBM)
    dma = pltpu.SemaphoreType.DMA
    flat = [x.reshape(1, -1) for x in (e1, o1, e2, o2, e3, o3)]
    shape = jax.ShapeDtypeStruct(troponin.shape, f32)
    operands = [
        pltpu.with_memory_space_constraint(x, pltpu.MemorySpace.HBM)
        for x in (calcium, activation, *flat, troponin, tension, unbind, relax)
    ]
    results = pl.pallas_call(
        functools.partial(kernel, sizes=sizes),
        out_shape=(shape, shape),
        in_specs=[hbm] * 12,
        out_specs=(vmem, vmem),
        scratch_shapes=[
            pltpu.VMEM(calcium.shape, f32),
            pltpu.VMEM(calcium.shape, f32),
            *[pltpu.VMEM(x.shape, x.dtype) for x in (*flat, troponin, tension, unbind, relax)],
            pltpu.VMEM((blocks, long, lanes), f32),
            pltpu.VMEM((short, lanes), f32),
            pltpu.VMEM((blocks + 1, subs + 1, lanes), f32),
            pltpu.VMEM((ny, long, lanes), f32),
            pltpu.VMEM((ny, short, lanes), f32),
            pltpu.VMEM((ny, subs + 1, lanes), f32),
            pltpu.VMEM((ny, subs + 1, lanes), f32),
            dma((2, subs)),
            dma((10,)),
            dma((blocks + 1, CHUNKS)),
            dma((blocks + 1,)),
            dma((ny, CHUNKS)),
            dma((ny, CHUNKS)),
            dma((ny,)),
            dma((ny,)),
        ],
        compiler_params=pltpu.CompilerParams(
            collective_id=0, has_side_effects=True, vmem_limit_bytes=32 * 1024 * 1024
        ),
        name="restrict_steps",
    )(*operands)
    results = [pltpu.with_memory_space_constraint(x, pltpu.MemorySpace.VMEM) for x in results]
    return pl.pallas_call(
        store_results,
        out_shape=(shape, shape),
        in_specs=[vmem] * 2,
        out_specs=(hbm, hbm),
        scratch_shapes=[dma((2,))],
        name="store_results",
    )(*results)


def solution(mesh):
    sizes = tuple(mesh.shape[name] for name in ("gx", "gy", "gz"))
    field = P(None, "gx", "gz", "gy")
    nodes = P("gx", ("gy", "gz"), None)
    return jax.shard_map(
        functools.partial(per_device, sizes=sizes),
        mesh=mesh,
        in_specs=(field, field, P(), P(), P(), P(), P(), P(), nodes, nodes, nodes, nodes),
        out_specs=(nodes, nodes),
        check_vma=False,
    )
```
